32 devices in a mesh: gossip: 8 (over z, x), mp: 4 (over y, core).
Axes of the slice: x: 2, y: 2, z: 4, core: 2. Of those that a mesh axis runs over, the one named last changes fastest.
Arguments:
- tokens: bfloat16 [8, 512, 2048], P('gossip'), may hold values from -6 to 6
- targets: bfloat16 [8, 512, 2048], P('gossip'), may hold values from -6 to 6
- gate_weight: bfloat16 [8, 2048, 4096], P('gossip', None, 'mp'), may hold values from -6 to 6
- up_weight: bfloat16 [8, 2048, 4096], P('gossip', None, 'mp'), may hold values from -6 to 6
- down_weight: bfloat16 [8, 4096, 2048], P('gossip', 'mp'), may hold values from -6 to 6
Outputs:
- gate_out: bfloat16 [8, 2048, 4096], P('gossip', None, 'mp')
- up_out: bfloat16 [8, 2048, 4096], P('gossip', None, 'mp')
- down_out: bfloat16 [8, 4096, 2048], P('gossip', 'mp')
The draws below stay inside these ranges and needn't reach their ends.
All inputs are finite; a program needn't handle non-finite values.
Results may differ from the reference program's by a relative error of at most 0.0095.
Values may be sent and summed in bfloat16 or wider, within the bound.
A program may use at most 128 MiB of HBM per device.

```python
import jax
import jax.numpy as jnp
from jax import lax

D = 2048
TOK = 512
ITERS = 1
FF = 4096
REPLICAS = 8


def levels(own_key, dims, pieces, least, largest):
    gain = 1.0
    for dim, blocks in pieces:
        steps = jax.random.uniform(jax.random.fold_in(jax.random.fold_in(own_key, 6), dim), (blocks,), jnp.float32, least / len(pieces), largest / len(pieces))
        gain = gain * jnp.repeat(jnp.exp(steps), dims[dim] // blocks).reshape((-1,) + (1,) * (len(dims) - 1 - dim))
    return gain


def bell_draw(stream_key, extent, spread, reach, split=(), kind=jnp.bfloat16):
    values = spread * jax.random.normal(stream_key, extent, jnp.float32)
    if split:
        values = values * levels(stream_key, extent, split, -0.22, 0.18)
    return jnp.clip(values, -reach, reach).astype(kind)


def setup_inputs(seed: int = 0) -> dict:
    keys = jax.random.split(jax.random.key(seed), 6)
    return {
        "tokens": bell_draw(keys[0], (REPLICAS, TOK, D), 1.0, 6.0, ((0, 8),)),
        "targets": bell_draw(keys[1], (REPLICAS, TOK, D), 1.0, 6.0, ((0, 8),)),
        "gate_weight": bell_draw(keys[2], (REPLICAS, D, FF), 1.0, 6.0, ((0, 8), (2, 4))),
        "up_weight": bell_draw(keys[3], (REPLICAS, D, FF), 1.0, 6.0, ((0, 8), (2, 4))),
        "down_weight": bell_draw(keys[4], (REPLICAS, FF, D), 1.0, 6.0, ((0, 8), (1, 4))),
    }


def rms_norm(values):
    widened = values.astype(jnp.float32)
    return (widened * lax.rsqrt(lax.optimization_barrier(jnp.mean(widened * widened, axis=-1, keepdims=True)) + 1e-06)).astype(jnp.bfloat16)

def mix_cycle(stepped):
    widened = stepped.astype(jnp.float32)
    total = jnp.roll(widened, 1, axis=0) + widened + jnp.roll(widened, -1, axis=0)
    return (total / 3.0).astype(jnp.bfloat16)

def reference(tokens, targets, gate_weight, up_weight, down_weight):
    tok_count = tokens.shape[1]
    width = tokens.shape[2]
    hidden_all = gate_weight.shape[2]
    in_scale = 1.0 / width ** 0.5
    mid_scale = 1.0 / hidden_all ** 0.5
    step_size = hidden_all / 4.0
    normed = rms_norm(tokens).astype(jnp.float32)
    offset = tokens.astype(jnp.float32) - targets.astype(jnp.float32)
    w_gate, w_up, w_down = (gate_weight, up_weight, down_weight)
    for iteration in range(ITERS):
        gate_pre = jnp.einsum('rtd,rdf->rtf', normed, w_gate.astype(jnp.float32)) * in_scale
        up_pre = jnp.einsum('rtd,rdf->rtf', normed, w_up.astype(jnp.float32)) * in_scale
        sig_gate = jax.nn.sigmoid(gate_pre)
        act_gate = gate_pre * sig_gate
        hidden = (act_gate * up_pre).astype(jnp.bfloat16).astype(jnp.float32)
        output = jnp.einsum('rtf,rfd->rtd', hidden, w_down.astype(jnp.float32)) * mid_scale
        err_grad = ((offset + output) / tok_count).astype(jnp.bfloat16).astype(jnp.float32)
        grad_down = jnp.einsum('rtf,rtd->rfd', hidden, err_grad) * mid_scale
        grad_hidden = jnp.einsum('rtd,rfd->rtf', err_grad, w_down.astype(jnp.float32)) * mid_scale
        grad_gate = (grad_hidden * up_pre * (sig_gate * (1.0 + gate_pre * (1.0 - sig_gate)))).astype(jnp.bfloat16).astype(jnp.float32)
        grad_up = (grad_hidden * act_gate).astype(jnp.bfloat16).astype(jnp.float32)
        grad_wgate = jnp.einsum('rtd,rtf->rdf', normed, grad_gate) * in_scale
        grad_wup = jnp.einsum('rtd,rtf->rdf', normed, grad_up) * in_scale
        new_gate = (w_gate.astype(jnp.float32) - step_size * grad_wgate).astype(jnp.bfloat16)
        new_up = (w_up.astype(jnp.float32) - step_size * grad_wup).astype(jnp.bfloat16)
        new_down = (w_down.astype(jnp.float32) - step_size * grad_down).astype(jnp.bfloat16)
        w_gate = mix_cycle(new_gate)
        w_up = mix_cycle(new_up)
        w_down = mix_cycle(new_down)
    return (w_gate, w_up, w_down)
```

```python
import jax
import jax.numpy as jnp
from jax import lax
from jax.sharding import PartitionSpec as P

ITERS = 1


def passed_along(value, axis, steps):
    count = lax.axis_size(axis)
    pairs = [(source, (source + steps) % count) for source in range(count)]
    return lax.ppermute(value, axis, pairs)


def rms_norm(values):
    widened = values.astype(jnp.float32)
    return (
        widened * lax.rsqrt(jnp.mean(widened * widened, axis=-1, keepdims=True) + 1e-06)
    ).astype(jnp.bfloat16)


def mix_three(lower, own, upper):
    total = lower.astype(jnp.float32) + own.astype(jnp.float32) + upper.astype(jnp.float32)
    return (total / 3.0).astype(jnp.bfloat16)


def neighbours_sum_mix(own, axis):
    count = lax.axis_size(axis)
    if count % 2 or count < 4:
        return mix_three(passed_along(own, axis, 1), own, passed_along(own, axis, -1))
    swap = [(r, r ^ 1) for r in range(count)]
    onward = [(r, (r + 2) % count if r % 2 == 0 else (r - 2) % count) for r in range(count)]
    partner = lax.ppermute(own, axis, swap)
    far = lax.ppermute(partner, axis, onward)
    return mix_three(partner, own, far)


CHUNKS = 4


def chunk_rows(rows):
    size = rows // CHUNKS
    return [(i * size, size) for i in range(CHUNKS)]


def assemble(pieces, shape):
    out = jnp.zeros(shape, jnp.bfloat16)
    at = 0
    for piece in pieces:
        out = lax.dynamic_update_slice_in_dim(out, piece, at, 0)
        at += piece.shape[0]
    return out


def local(tokens, targets, gate_weight, up_weight, down_weight):
    inputs = tokens[0]
    wanted = targets[0]
    w_gate = gate_weight[0]
    w_up = up_weight[0]
    w_down = down_weight[0]
    gate_shape = w_gate.shape
    down_shape = w_down.shape
    tok_count = inputs.shape[0]
    width = inputs.shape[1]
    mp_count = lax.axis_size("mp")
    hidden_all = w_gate.shape[1] * mp_count
    in_scale = 1.0 / width**0.5
    mid_scale = 1.0 / hidden_all**0.5
    step_size = hidden_all / 4.0
    normed = rms_norm(inputs)
    offset = inputs.astype(jnp.float32) - wanted.astype(jnp.float32)
    own_rows = tok_count // mp_count
    offset_own = lax.dynamic_slice_in_dim(offset, lax.axis_index("mp") * own_rows, own_rows, 0)
    for iteration in range(ITERS):
        gate_pre = jnp.dot(normed, w_gate, preferred_element_type=jnp.float32) * in_scale
        up_pre = jnp.dot(normed, w_up, preferred_element_type=jnp.float32) * in_scale
        sig_gate = jax.nn.sigmoid(gate_pre)
        act_gate = gate_pre * sig_gate
        hidden = (act_gate * up_pre).astype(jnp.bfloat16)
        partial_value = jnp.dot(hidden, w_down, preferred_element_type=jnp.float32)
        output_own = (
            lax.psum_scatter(
                partial_value.astype(jnp.bfloat16), "mp", scatter_dimension=0, tiled=True
            ).astype(jnp.float32)
            * mid_scale
        )
        err_own = ((offset_own + output_own) / tok_count).astype(jnp.bfloat16)
        err_grad = lax.all_gather(err_own, "mp", axis=0, tiled=True)
        downs = []
        for at, size in chunk_rows(down_shape[0]):
            grad = jnp.einsum(
                "tf,td->fd", hidden[:, at : at + size], err_grad, preferred_element_type=jnp.float32
            ) * mid_scale
            old = w_down[at : at + size]
            new = (old.astype(jnp.float32) - step_size * grad).astype(jnp.bfloat16)
            downs.append(neighbours_sum_mix(new, "gossip"))
        grad_hidden = (
            jnp.einsum("td,fd->tf", err_grad, w_down, preferred_element_type=jnp.float32)
            * mid_scale
        )
        grad_gate = (
            grad_hidden * up_pre * (sig_gate * (1.0 + gate_pre * (1.0 - sig_gate)))
        ).astype(jnp.bfloat16)
        grad_up = (grad_hidden * act_gate).astype(jnp.bfloat16)
        mixed = []
        for grads, weights in ((grad_gate, w_gate), (grad_up, w_up)):
            pieces = []
            for at, size in chunk_rows(gate_shape[0]):
                grad = jnp.einsum(
                    "td,tf->df", normed[:, at : at + size], grads, preferred_element_type=jnp.float32
                ) * in_scale
                old = weights[at : at + size]
                new = (old.astype(jnp.float32) - step_size * grad).astype(jnp.bfloat16)
                pieces.append(neighbours_sum_mix(new, "gossip"))
            mixed.append(assemble(pieces, gate_shape))
        w_gate, w_up = mixed
        w_down = assemble(downs, down_shape)
    return (w_gate[None], w_up[None], w_down[None])


def solution(mesh):
    placed = (
        P("gossip", None, None),
        P("gossip", None, None),
        P("gossip", None, "mp"),
        P("gossip", None, "mp"),
        P("gossip", "mp", None),
    )
    return jax.shard_map(
        local,
        mesh=mesh,
        in_specs=placed,
        out_specs=(P("gossip", None, "mp"), P("gossip", None, "mp"), P("gossip", "mp", None)),
        check_vma=False,
    )
```

```python
import jax
import jax.numpy as jnp
from jax import lax
from jax.sharding import PartitionSpec as P

ITERS = 1


def passed_along(value, axis, steps):
    count = lax.axis_size(axis)
    pairs = [(source, (source + steps) % count) for source in range(count)]
    return lax.ppermute(value, axis, pairs)


def rms_norm(values):
    widened = values.astype(jnp.float32)
    return (
        widened * lax.rsqrt(jnp.mean(widened * widened, axis=-1, keepdims=True) + 1e-06)
    ).astype(jnp.bfloat16)


def mix_three(lower, own, upper):
    total = lower.astype(jnp.float32) + own.astype(jnp.float32) + upper.astype(jnp.float32)
    return (total / 3.0).astype(jnp.bfloat16)


class Exchange:
    def __init__(self, axis):
        self.axis = axis
        self.count = lax.axis_size(axis)
        self.number = 0

    def both(self, own, step=None):
        count, axis = (self.count, self.axis)
        if step is None:
            step = self.number
            self.number += 1
        if count % 2 or count < 4:
            lower = passed_along(own, axis, 1)
            return lower, passed_along(own, axis, -1)
        swap = [(r, r ^ 1) for r in range(count)]
        onward = [(r, (r + 2) % count if r % 2 == 0 else (r - 2) % count) for r in range(count)]
        partner = lax.ppermute(own, axis, swap)
        far = lax.ppermute(partner, axis, onward)
        return partner, far

    def mix(self, own):
        partner, far = self.both(own)
        return mix_three(partner, own, far)


EVEN = (2, 2, 2, 2)
TAPER = (2, 2, 2, 1, 1)
GATE_PARTS = (1, 1)


def cuts(rows, parts):
    at = 0
    for part in parts:
        size = rows * part // sum(parts)
        yield at, size
        at += size


def halving_sum(value, axis):
    count = lax.axis_size(axis)
    rows, width = (value.shape[0] // count, value.shape[1])
    if count & (count - 1):
        return lax.psum_scatter(
            value.astype(jnp.bfloat16), axis, scatter_dimension=0, tiled=True
        ).astype(jnp.float32)
    index = lax.axis_index(axis)
    bit = 1
    while bit < count:
        value = value.reshape(-1, 2, rows, width)
        side = jnp.where(index & bit, 1, 0)
        kept = lax.dynamic_index_in_dim(value, side, 1, keepdims=False)
        given = lax.dynamic_index_in_dim(value, 1 - side, 1, keepdims=False).astype(jnp.bfloat16)
        came = lax.ppermute(given, axis, [(r, r ^ bit) for r in range(count)])
        value = kept.astype(jnp.float32) + came.astype(jnp.float32)
        bit *= 2
    return value.reshape(rows, width)


def doubling_gather(value, axis):
    count = lax.axis_size(axis)
    if count & (count - 1):
        return lax.all_gather(value, axis, axis=0, tiled=True)
    rows, width = value.shape
    index = lax.axis_index(axis)
    value = value[None]
    bit = count // 2
    while bit:
        came = lax.ppermute(value, axis, [(r, r ^ bit) for r in range(count)])
        high = (index & bit) != 0
        first = jnp.where(high, came, value)
        second = jnp.where(high, value, came)
        value = jnp.stack([first, second], axis=1).reshape(-1, rows, width)
        bit //= 2
    return value.reshape(count * rows, width)


def assemble(pieces, shape):
    out = jnp.zeros(shape, jnp.bfloat16)
    at = 0
    for piece in pieces:
        out = lax.dynamic_update_slice_in_dim(out, piece, at, 0)
        at += piece.shape[0]
    return out


def local(tokens, targets, gate_weight, up_weight, down_weight):
    inputs = tokens[0]
    wanted = targets[0]
    w_gate = gate_weight[0]
    w_up = up_weight[0]
    w_down = down_weight[0]
    gate_shape = w_gate.shape
    down_shape = w_down.shape
    tok_count = inputs.shape[0]
    width = inputs.shape[1]
    mp_count = lax.axis_size("mp")
    hidden_all = w_gate.shape[1] * mp_count
    in_scale = 1.0 / width**0.5
    mid_scale = 1.0 / hidden_all**0.5
    step_size = hidden_all / 4.0
    normed = rms_norm(inputs)
    offset = inputs.astype(jnp.float32) - wanted.astype(jnp.float32)
    own_rows = tok_count // mp_count
    offset_own = lax.dynamic_slice_in_dim(offset, lax.axis_index("mp") * own_rows, own_rows, 0)
    shared = w_gate.shape[1] * 5 // 8 // 128 * 128
    for _ in range(ITERS):
        exchange = Exchange("gossip")
        normed_own = lax.dynamic_slice_in_dim(
            normed, lax.axis_index("mp") * own_rows, own_rows, 0
        )
        near_normed = exchange.both(normed_own, "a")
        half = gate_shape[0] // 2
        near_top = exchange.both(w_gate[:half, :shared], "b")
        near_low = exchange.both(w_gate[half:, :shared], "c")
        gate_pre = jnp.dot(normed, w_gate, preferred_element_type=jnp.float32) * in_scale
        up_pre = jnp.dot(normed, w_up, preferred_element_type=jnp.float32) * in_scale
        sig_gate = jax.nn.sigmoid(gate_pre)
        act_gate = gate_pre * sig_gate
        hidden = (act_gate * up_pre).astype(jnp.bfloat16)
        partial_value = jnp.dot(hidden, w_down, preferred_element_type=jnp.float32)
        output_own = halving_sum(partial_value, "mp") * mid_scale
        err_own = ((offset_own + output_own) / tok_count).astype(jnp.bfloat16)
        err_grad = doubling_gather(err_own, "mp")
        downs = []
        for at, size in cuts(down_shape[0], EVEN):
            grad = jnp.einsum(
                "tf,td->fd", hidden[:, at : at + size], err_grad, preferred_element_type=jnp.float32
            ) * mid_scale
            old = w_down[at : at + size]
            new = (old.astype(jnp.float32) - step_size * grad).astype(jnp.bfloat16)
            downs.append(exchange.mix(new))
        grad_hidden = (
            jnp.einsum("td,fd->tf", err_grad, w_down, preferred_element_type=jnp.float32)
            * mid_scale
        )
        grad_gate = (
            grad_hidden * up_pre * (sig_gate * (1.0 + gate_pre * (1.0 - sig_gate)))
        ).astype(jnp.bfloat16)
        grad_up = (grad_hidden * act_gate).astype(jnp.bfloat16)
        near_grads = exchange.both(grad_gate[:, :shared])

        def stepped(old, inputs_t, grads):
            grad = (
                jnp.einsum("td,tf->df", inputs_t, grads, preferred_element_type=jnp.float32)
                * in_scale
            )
            return (old.astype(jnp.float32) - step_size * grad).astype(jnp.bfloat16)

        rest = []
        for at, size in cuts(gate_shape[0], GATE_PARTS):
            new = stepped(
                w_gate[at : at + size, shared:], normed[:, at : at + size], grad_gate[:, shared:]
            )
            rest.append(exchange.mix(new))
        ups = []
        for at, size in cuts(gate_shape[0], TAPER):
            new = stepped(w_up[at : at + size], normed[:, at : at + size], grad_up)
            ups.append(exchange.mix(new))
        gathered = []
        for side in range(2):
            piece, _ = lax.optimization_barrier((near_normed[side], err_grad))
            gathered.append(doubling_gather(piece, "mp"))
        fronts = []
        for at, tops in ((0, near_top), (half, near_low)):
            own = stepped(
                w_gate[at : at + half, :shared],
                normed[:, at : at + half],
                grad_gate[:, :shared],
            )
            others = [
                stepped(tops[i], gathered[i][:, at : at + half], near_grads[i]) for i in range(2)
            ]
            fronts.append(mix_three(others[0], own, others[1]))
        mixed_gate = jnp.zeros(gate_shape, jnp.bfloat16)
        for pieces, column in ((fronts, 0), (rest, shared)):
            at = 0
            for piece in pieces:
                mixed_gate = lax.dynamic_update_slice(mixed_gate, piece, (at, column))
                at += piece.shape[0]
        w_gate = mixed_gate
        w_up = assemble(ups, gate_shape)
        w_down = assemble(downs, down_shape)
    return (w_gate[None], w_up[None], w_down[None])


def solution(mesh):
    placed = (
        P("gossip", None, None),
        P("gossip", None, None),
        P("gossip", None, "mp"),
        P("gossip", None, "mp"),
        P("gossip", "mp", None),
    )
    return jax.shard_map(
        local,
        mesh=mesh,
        in_specs=placed,
        out_specs=(P("gossip", None, "mp"), P("gossip", None, "mp"), P("gossip", "mp", None)),
        check_vma=False,
    )
```
